32 devices in a mesh: tm: 8 (over y, x, core), space: 4 (over z).
Axes of the slice: x: 2, y: 2, z: 4, core: 2. Of those that a mesh axis runs over, the one named last changes fastest.
Arguments:
- initial_state: float32 [1024, 1024], P('space'), may hold values from -6 to 6
- guess_coarse: float32 [8, 1024, 1024], P('tm', 'space'), may hold values from -6 to 6
- force_fine: float32 [8, 1024, 1024], P('tm', 'space'), may hold values from -6 to 6
- force_coarse: float32 [8, 1024, 1024], P('tm', 'space'), may hold values from -6 to 6
- eigen_basis: float32 [1024, 1024], replicated, may hold values from -1 to 1, as said below
- eigen_rates: float32 [1024], replicated, may hold values from 0.02 to 4
- carried_correction: float32 [1024, 1024], replicated, may hold values from -6 to 6
Outputs:
- fine_states: float32 [8, 1024, 1024], P('tm', 'space')
- coarse_states: float32 [8, 1024, 1024], P('tm', 'space')
The draws below stay inside these ranges and needn't reach their ends.
Inputs may be any that keep to these rules, and one draw needn't show every extreme that they name: `eigen_basis`: an orthogonal matrix: its transpose is its inverse up to float32 rounding.
All inputs are finite; a program needn't handle non-finite values.
Results may differ from the reference program's by a relative error of at most 0.00013.
Values sent between devices are 32-bit elements; how exact they have to be, the bound alone decides.
A program may use at most 128 MiB of HBM per device.

```python
import math
import jax
import jax.numpy as jnp
from jax import lax

GRID = 1024
GROUPS = 8


def draw_eigen_basis(key, part):
    skewed = jax.random.normal(key, (GRID, GRID), jnp.float32) / math.sqrt(GRID)
    skewed = skewed - skewed.T
    identity = jnp.eye(GRID, dtype=jnp.float32)
    return jnp.linalg.solve(identity + skewed, identity - skewed)


def shard_levels(stream_key, dims, split, least, high):
    level = 1.0
    for dim, shards_of in split:
        heights = jax.random.uniform(jax.random.fold_in(jax.random.fold_in(stream_key, 6), dim), (shards_of,), jnp.float32, least / len(split), high / len(split))
        level = level * jnp.repeat(jnp.exp(heights), dims[dim] // shards_of).reshape((-1,) + (1,) * (len(dims) - 1 - dim))
    return level


def scatter_about(key, shape, scale, most, pieces=(), kind=jnp.bfloat16):
    loudness = shard_levels(key, shape, pieces, -0.22, 0.18) if pieces else 1.0
    array = jax.random.normal(key, shape, jnp.float32) * scale * loudness
    return jnp.minimum(jnp.maximum(array, -most), most).astype(kind)


def setup_inputs(seed: int = 0) -> dict:
    key_of = jax.random.split(jax.random.key(seed), 8)
    return {
        "initial_state": scatter_about(key_of[0], (GRID, GRID), 1.0, 6.0, ((0, 4),), jnp.float32),
        "guess_coarse": scatter_about(key_of[1], (GROUPS, GRID, GRID), 1.0, 6.0, ((0, 8), (1, 4)), jnp.float32),
        "force_fine": scatter_about(key_of[2], (GROUPS, GRID, GRID), 1.0, 6.0, ((0, 8), (1, 4)), jnp.float32),
        "force_coarse": scatter_about(key_of[3], (GROUPS, GRID, GRID), 1.0, 6.0, ((0, 8), (1, 4)), jnp.float32),
        "eigen_basis": draw_eigen_basis(jax.random.fold_in(key_of[7], 71), 0),
        "eigen_rates": jnp.clip(jnp.exp(jax.random.uniform(key_of[5], (GRID,), jnp.float32, math.log(0.02), math.log(4.0))), 0.02, 4.0),
        "carried_correction": scatter_about(key_of[6], (GRID, GRID), 1.0, 6.0, (), jnp.float32),
    }


exact_mode = lax.Precision.HIGHEST

def reference(initial_state, guess_coarse, force_fine, force_coarse, eigen_basis, eigen_rates, carried_correction):
    fine_decay = 1.0 / (1.0 + eigen_rates[:, None] + eigen_rates[None, :])
    coarse_decay = 1.0 / (1.0 + 2.0 * (eigen_rates[:, None] + eigen_rates[None, :]))

    def to_eigen(field):
        right = jnp.einsum('gij,jk->gik', field, eigen_basis, precision=exact_mode)
        return jnp.einsum('ji,gjk->gik', eigen_basis, right, precision=exact_mode)

    def from_eigen(coeffs):
        left = jnp.einsum('ij,gjk->gik', eigen_basis, coeffs, precision=exact_mode)
        return jnp.einsum('gij,kj->gik', left, eigen_basis, precision=exact_mode)

    def reaction(field):
        return field + 0.5 * jnp.tanh(field)

    def propagate(field, source):
        return from_eigen(fine_decay[None] * to_eigen(reaction(field) + source))

    def previous(states):
        return jnp.concatenate([initial_state[None], states[:-1]], axis=0)
    relaxed_fine = propagate(previous(guess_coarse), force_fine)
    relaxed_coarse = propagate(relaxed_fine, force_coarse)
    second_fine = propagate(previous(relaxed_coarse), force_fine)
    residual = fine_decay[None] * to_eigen(reaction(second_fine) + force_coarse) - to_eigen(relaxed_coarse)

    def coarse_turn(carry, term):
        updated = coarse_decay * carry + term
        return (updated, updated)
    unused, correction = lax.scan(coarse_turn, carried_correction, residual)
    coarse_states = relaxed_coarse + from_eigen(correction)
    fine_states = propagate(previous(coarse_states), force_fine)
    return (fine_states, coarse_states)
```

```python
import jax
import jax.numpy as jnp
from jax import lax
from jax.sharding import PartitionSpec as P

mode = lax.Precision.HIGH


def product(left, right):
    return jnp.dot(left, right, preferred_element_type=jnp.float32, precision=mode)


def reaction(field):
    return field + 0.5 * jnp.tanh(field)


def decay_block(eigen_rates, own_rates, factor):
    return 1.0 / (1.0 + factor * (eigen_rates[:, None] + own_rates[None, :]))


def shift(block, distance):
    count = lax.axis_size("tm")
    return lax.ppermute(block, "tm", [(i, (i + distance) % count) for i in range(count)])


def swap(block):
    count = lax.axis_size("tm")
    return lax.ppermute(block, "tm", [(i, i ^ 1) for i in range(count)])


def to_eigen(field, basis, basis_t):
    right = product(field, basis)
    columns = lax.all_to_all(right, "space", split_axis=1, concat_axis=0, tiled=True)
    return product(basis_t, columns)


def from_eigen(coeffs, basis, basis_t):
    left = product(basis, coeffs)
    rows = lax.all_to_all(left, "space", split_axis=0, concat_axis=1, tiled=True)
    return product(rows, basis_t)


def coarse_solve(terms, start, decay):
    count = lax.axis_size("tm")
    pairs = count // 2
    place = lax.axis_index("tm")
    pair, odd = place // 2, place % 2
    half = terms.shape[0] // 2

    def mine(block, which):
        return lax.dynamic_slice_in_dim(block, which * half, half, 0)

    other = swap(mine(terms, 1 - odd))
    own = mine(terms, odd)
    first = jnp.where(odd == 0, own, other)
    second = jnp.where(odd == 0, other, own)
    decay = mine(decay, odd)
    carried = mine(start, odd)
    is_last = pair == pairs - 1
    sums = second + decay * jnp.where(is_last, carried, first)
    squared = decay * decay
    before = jnp.where(is_last, sums, 0.0)
    arrived = {}
    for s in range(1, pairs):
        route = []
        for k in range(pairs):
            if s <= k + 1:
                source = (k - s) % pairs
                route += [(2 * source + c, 2 * k + c) for c in range(2)]
        arrived[s] = lax.ppermute(sums, "tm", route)
    for s in range(pairs - 1, 0, -1):
        before = squared * before + arrived[s]
    even_state = before
    odd_state = first + decay * even_state
    given = jnp.where(odd == 0, odd_state, even_state)
    kept = jnp.where(odd == 0, even_state, odd_state)
    got = swap(given)
    return jnp.where(
        odd == 0,
        jnp.concatenate([kept, got], 0),
        jnp.concatenate([got, kept], 0),
    )


def on_device(
    initial_state,
    guess_coarse,
    force_fine,
    force_coarse,
    eigen_basis,
    eigen_rates,
    carried_correction,
):
    row_count = initial_state.shape[0]
    offset = lax.axis_index("space") * row_count
    own_rates = lax.dynamic_slice_in_dim(eigen_rates, offset, row_count, 0)
    fine_decay = decay_block(eigen_rates, own_rates, 1.0)
    coarse_decay = decay_block(eigen_rates, own_rates, 2.0)
    carried = lax.dynamic_slice_in_dim(carried_correction, offset, row_count, 1)
    place = lax.axis_index("tm")
    at_start = place == 0
    at_end = place == lax.axis_size("tm") - 1
    fine_here, coarse_here = force_fine[0], force_coarse[0]
    fine_next, coarse_next = shift(fine_here, -1), shift(coarse_here, -1)
    basis, basis_t = eigen_basis, eigen_basis.T

    def relax(field, source):
        return fine_decay * to_eigen(reaction(field) + source, basis, basis_t)

    def field_of(coeffs):
        return from_eigen(coeffs, basis, basis_t)

    entering = jnp.where(at_start, initial_state, shift(guess_coarse[0], 1))
    relaxed_fine = field_of(relax(entering, fine_here))
    relaxed = relax(relaxed_fine, coarse_here)
    relaxed_coarse = jnp.where(at_end, initial_state, field_of(relaxed))
    second_fine = field_of(relax(relaxed_coarse, fine_next))
    target = relax(second_fine, coarse_next)
    terms = target - jnp.where(at_end, 0.0, coarse_decay * relaxed)
    states = coarse_solve(terms, carried, coarse_decay)
    coarse_new = field_of(states)
    fine_new = field_of(relax(jnp.where(at_end, initial_state, coarse_new), fine_next))
    return (shift(fine_new, 1)[None], coarse_new[None])


def solution(mesh):
    placed = (
        P("space", None),
        P("tm", "space", None),
        P("tm", "space", None),
        P("tm", "space", None),
        P(),
        P(),
        P(),
    )
    return jax.shard_map(
        on_device,
        mesh=mesh,
        in_specs=placed,
        out_specs=(P("tm", "space", None), P("tm", "space", None)),
        check_vma=False,
    )
```

```python
import functools
import jax
import jax.numpy as jnp
from jax import lax
from jax.experimental import pallas as pl
from jax.experimental.pallas import tpu as pltpu
from jax.sharding import PartitionSpec as P

mode = lax.Precision.HIGHEST


def halves(block):
    high = block.astype(jnp.bfloat16)
    return high, (block - high.astype(jnp.float32)).astype(jnp.bfloat16)


def dot3(left, right):
    dot = functools.partial(jnp.dot, preferred_element_type=jnp.float32)
    return dot(left[0], right[0]) + dot(left[0], right[1]) + dot(left[1], right[0])


def stages_kernel(
    plan, forced, basis, basis_t, decay, start, sources, fixed, outs, split, split_tall, field, coeffs, sent, held, send_sem, recv_sem
):
    count = lax.axis_size("space")
    me = lax.axis_index("space")
    rows = held.shape[2]
    barrier = pltpu.get_barrier_semaphore()

    @pl.loop(0, count)
    def _(d):
        @pl.when(d != me)
        def _():
            pl.semaphore_signal(barrier, inc=1, device_id={"space": d}, device_id_type=pl.DeviceIdType.MESH)

    pl.semaphore_wait(barrier, count - 1)

    def span(d):
        return pl.ds(pl.multiple_of(d * rows, rows), rows)

    def peer(k):
        return jnp.where(me < count // 2, count - 1 - k, k)

    def copy(stage, d):
        return pltpu.make_async_remote_copy(
            src_ref=sent.at[stage, d],
            dst_ref=held.at[stage, me],
            send_sem=send_sem.at[stage, d],
            recv_sem=recv_sem.at[stage, me],
            device_id={"space": d},
            device_id_type=pl.DeviceIdType.MESH,
        )

    def arrival(stage, s):
        return pltpu.make_async_remote_copy(
            src_ref=sent.at[stage, s],
            dst_ref=held.at[stage, s],
            send_sem=send_sem.at[stage, s],
            recv_sem=recv_sem.at[stage, s],
            device_id={"space": s},
            device_id_type=pl.DeviceIdType.MESH,
        )

    def exchange(stage, block_for, use):
        @pl.loop(0, count)
        def _(k):
            d = peer(k)
            block = block_for(d)

            @pl.when(d != me)
            def _():
                sent[stage, d] = block
                copy(stage, d).start()

            @pl.when(d == me)
            def _():
                held[stage, me] = block

        use(me, True)

        @pl.loop(0, count)
        def _(k):
            s = peer(k)

            @pl.when(s != me)
            def _():
                arrival(stage, s).wait_recv()
                use(s, False)

    def forward(stage):
        high, low = halves(field[...])
        split[0] = high
        split[1] = low

        def block_for(d):
            return dot3((split[0], split[1]), (basis[0, :, span(d)], basis[1, :, span(d)]))

        def use(s, first):
            part = halves(held[stage, s])

            @pl.loop(0, count)
            def _(r):
                term = dot3((basis_t[0, span(r), span(s)], basis_t[1, span(r), span(s)]), part)
                coeffs[span(r), :] = term if first else coeffs[span(r), :] + term

        exchange(stage, block_for, use)

    def inverse(stage):
        high, low = halves(coeffs[...])
        split_tall[0] = high
        split_tall[1] = low

        def block_for(d):
            return dot3((basis[0, span(d), :], basis[1, span(d), :]), (split_tall[0], split_tall[1]))

        def use(s, first):
            part = halves(held[stage, s])

            @pl.loop(0, count)
            def _(r):
                term = dot3(part, (basis_t[0, span(s), span(r)], basis_t[1, span(s), span(r)]))
                field[:, span(r)] = term if first else field[:, span(r)] + term

        exchange(stage, block_for, use)

    def react(source):
        value = field[...]
        field[...] = value + 0.5 * jnp.tanh(value) + source[...]

    sources = list(sources)
    outs = list(outs)
    if plan[0] == "E":
        field[...] = start[...]
        react(sources.pop(0))
    else:
        coeffs[...] = start[...]
    for stage, kind in enumerate(plan):
        final = stage == len(plan) - 1
        if kind == "E":
            forward(stage)
            coeffs[...] = coeffs[...] * decay[...]
            if stage in forced:
                outs.pop(0)[...] = coeffs[...]
        else:
            inverse(stage)
            if stage in forced:
                outs.pop(0)[...] = field[...]
            if not final:
                if fixed is not None:
                    @pl.when(lax.axis_index("tm") == lax.axis_size("tm") - 1)
                    def _():
                        field[...] = fixed[...]
                react(sources.pop(0))

    for stage in range(len(plan)):
        @pl.loop(0, count)
        def _(d):
            @pl.when(d != me)
            def _():
                copy(stage, d).wait_send()


def stages(plan, forced, number, basis, basis_t, decay, start, sources, fixed=None):
    grid, rows = decay.shape
    count = grid // rows
    wide, tall = (rows, grid), (grid, rows)
    extra = 0 if fixed is None else 1
    shapes = [jax.ShapeDtypeStruct(tall if plan[s] == "E" else wide, jnp.float32) for s in forced]

    def kernel(*refs):
        refs = list(refs)
        basis_ref, basis_t_ref, decay_ref, start_ref = refs[:4]
        del refs[:4]
        source_refs = refs[: len(sources)]
        del refs[: len(sources)]
        fixed_ref = refs.pop(0) if extra else None
        out_refs = refs[: len(shapes)]
        stages_kernel(
            plan, forced, basis_ref, basis_t_ref, decay_ref, start_ref, source_refs, fixed_ref, out_refs, *refs[len(shapes):]
        )

    operands = [basis, basis_t, decay, start, *sources] + ([fixed] if extra else [])
    steps = len(plan)
    vmem = pl.BlockSpec(memory_space=pltpu.VMEM)
    return pl.pallas_call(
        kernel,
        out_shape=shapes,
        in_specs=[vmem] * len(operands),
        out_specs=[vmem] * len(shapes),
        scratch_shapes=[
            pltpu.VMEM((2, *wide), jnp.bfloat16),
            pltpu.VMEM((2, *tall), jnp.bfloat16),
            pltpu.VMEM(wide, jnp.float32),
            pltpu.VMEM(tall, jnp.float32),
            pltpu.VMEM((steps, count, rows, rows), jnp.float32),
            pltpu.VMEM((steps, count, rows, rows), jnp.float32),
            pltpu.SemaphoreType.DMA((steps, count)),
            pltpu.SemaphoreType.DMA((steps, count)),
        ],
        compiler_params=pltpu.CompilerParams(
            collective_id=number, has_side_effects=True, vmem_limit_bytes=48 * 1024 * 1024
        ),
        cost_estimate=pl.CostEstimate(
            flops=steps * 40_000_000_000, bytes_accessed=8 * grid * grid, transcendentals=0
        ),
        name="stages_%d" % number,
    )(*operands)


def product(left, right):
    return jnp.dot(left, right, preferred_element_type=jnp.float32, precision=mode)


def reaction(field):
    return field + 0.5 * jnp.tanh(field)


def decay_block(eigen_rates, own_rates, factor):
    return 1.0 / (1.0 + factor * (eigen_rates[:, None] + own_rates[None, :]))


def shift(block, distance):
    count = lax.axis_size("tm")
    return lax.ppermute(block, "tm", [(i, (i + distance) % count) for i in range(count)])


def swap(block):
    count = lax.axis_size("tm")
    return lax.ppermute(block, "tm", [(i, i ^ 1) for i in range(count)])


def coarse_solve(terms, start, decay):
    count = lax.axis_size("tm")
    pairs = count // 2
    place = lax.axis_index("tm")
    pair, odd = place // 2, place % 2
    half = terms.shape[0] // 2

    def mine(block, which):
        return lax.dynamic_slice_in_dim(block, which * half, half, 0)

    other = swap(mine(terms, 1 - odd))
    own = mine(terms, odd)
    first = jnp.where(odd == 0, own, other)
    second = jnp.where(odd == 0, other, own)
    decay = mine(decay, odd)
    carried = mine(start, odd)
    is_last = pair == pairs - 1
    sums = second + decay * jnp.where(is_last, carried, first)
    squared = decay * decay
    before = jnp.where(is_last, sums, 0.0)
    arrived = {}
    for s in range(1, pairs):
        route = []
        for k in range(pairs):
            if s <= k + 1:
                source = (k - s) % pairs
                route += [(2 * source + c, 2 * k + c) for c in range(2)]
        arrived[s] = lax.ppermute(sums, "tm", route)
    for s in range(pairs - 1, 0, -1):
        before = squared * before + arrived[s]
    even_state = before
    odd_state = first + decay * even_state
    given = jnp.where(odd == 0, odd_state, even_state)
    kept = jnp.where(odd == 0, even_state, odd_state)
    got = swap(given)
    return jnp.where(
        odd == 0,
        jnp.concatenate([kept, got], 0),
        jnp.concatenate([got, kept], 0),
    )


def on_device(
    initial_state,
    guess_coarse,
    force_fine,
    force_coarse,
    eigen_basis,
    eigen_rates,
    carried_correction,
):
    row_count = initial_state.shape[0]
    offset = lax.axis_index("space") * row_count
    own_rates = lax.dynamic_slice_in_dim(eigen_rates, offset, row_count, 0)
    fine_decay = decay_block(eigen_rates, own_rates, 1.0)
    coarse_decay = decay_block(eigen_rates, own_rates, 2.0)
    carried = lax.dynamic_slice_in_dim(carried_correction, offset, row_count, 1)
    place = lax.axis_index("tm")
    at_start = place == 0
    at_end = place == lax.axis_size("tm") - 1
    fine_here, coarse_here = force_fine[0], force_coarse[0]
    fine_next, coarse_next = shift(fine_here, -1), shift(coarse_here, -1)
    high = lax.reduce_precision(eigen_basis, 8, 7)
    basis = jnp.stack([high, eigen_basis - high]).astype(jnp.bfloat16)
    basis_t = jnp.swapaxes(basis, 1, 2)
    run = functools.partial(stages, basis=basis, basis_t=basis_t, decay=fine_decay)

    entering = jnp.where(at_start, initial_state, shift(guess_coarse[0], 1))
    relaxed, relaxed_coarse = run("EIEI", (2, 3), 1, start=entering, sources=[fine_here, coarse_here])
    gathered = product(eigen_basis.T, product(eigen_basis, relaxed)) - relaxed
    from_here = jnp.where(at_end, initial_state, relaxed_coarse)
    (target,) = run("EIE", (2,), 2, start=from_here, sources=[fine_next, coarse_next])
    terms = target - jnp.where(at_end, 0.0, coarse_decay * (relaxed + gathered))
    states = coarse_solve(terms, carried, coarse_decay) - gathered
    coarse_new, fine_new = run("IEI", (0, 2), 3, start=states, sources=[fine_next], fixed=initial_state)
    return (shift(fine_new, 1)[None], coarse_new[None])


def solution(mesh):
    placed = (
        P("space", None),
        P("tm", "space", None),
        P("tm", "space", None),
        P("tm", "space", None),
        P(),
        P(),
        P(),
    )
    return jax.shard_map(
        on_device,
        mesh=mesh,
        in_specs=placed,
        out_specs=(P("tm", "space", None), P("tm", "space", None)),
        check_vma=False,
    )
```
